32 devices in a mesh: gx: 4 (over y, core), gy: 2 (over x), gz: 4 (over z).
Axes of the slice: x: 2, y: 2, z: 4, core: 2. Of those that a mesh axis runs over, the one named last changes fastest.
Arguments:
- positions: float32 [3, 4096, 128], P(None, ('gx', 'gy', 'gz')), may hold values from 0 to 1, as said below
- charges: float32 [4096, 128], P(('gx', 'gy', 'gz')), may hold values from -6 to 6
- velocities: float32 [3, 4096, 128], P(None, ('gx', 'gy', 'gz')), may hold values from -6 to 6
- leaf_ids: int32 [4096], P(('gx', 'gy', 'gz')), may hold values from 0 to 2097151, as said below
- live_counts: int32 [32], replicated, may hold values from 32 to 96
- send_counts: int32 [5, 32], replicated, may hold values from 0 to 32, as said below
Outputs:
- moved_positions: float32 [3, 4096, 128], P(None, ('gx', 'gy', 'gz'))
- moved_charges: float32 [4096, 128], P(('gx', 'gy', 'gz'))
- moved_velocities: float32 [3, 4096, 128], P(None, ('gx', 'gy', 'gz'))
- moved_leaves: int32 [4096], P(('gx', 'gy', 'gz'))
- leaf_moments: float32 [286, 4096], P(None, ('gx', 'gy', 'gz'))
- parent_moments: float32 [286, 4096], P(None, ('gx', 'gy', 'gz'))
The draws below stay inside these ranges and needn't reach their ends.
Inputs may be any that keep to these rules, and one draw needn't show every extreme that they name: `positions`: every particle of a live slot lies inside the leaf cell of side 2^-7 named by the slot's leaf index. `leaf_ids`: morton indices of cells at depth 7; a leaf's parent cell is its index // 8. `send_counts`: no device sends more blocks than it holds live; after every section no device holds more than 128 live blocks; in every draw some device sends exactly 32 blocks in the first section and its partner then holds exactly 128.
All inputs are finite; a program needn't handle non-finite values.
Results may differ from the reference program's by a relative error of at most 0.0003.
Values sent between devices are 32-bit elements; how exact they have to be, the bound alone decides.
No kernel may reach another device: no remote copies, remote signals or barrier semaphores. Data moves between devices by JAX's collectives and lax.ppermute only.
A program may use at most 128 MiB of HBM per device.

```python
import math
from functools import partial
import jax
import jax.numpy as jnp
import numpy as np
from jax import lax

CAP = 128
PART = 128
ORDER = 10
LEVEL = 7
SEND_CAP = 32
SECTIONS = 5
NCOEF = 286
BLOCKS = 4096
N_GX = 4
N_GY = 2
DEVICES = 32


def leaf_table(key):
    base_key = jax.random.fold_in(key, 11)
    climb_key, start_key, octant_key, order_key = jax.random.split(base_key, 4)
    climbs = (jax.random.randint(climb_key, (DEVICES, CAP), 0, 3) == 0).astype(jnp.int32)
    parents = jax.random.randint(start_key, (DEVICES, 1), 0, 8 ** (LEVEL - 1) - CAP) + jnp.cumsum(climbs, axis=1)
    row_keys = jax.random.split(order_key, DEVICES)
    parents = jax.vmap(jax.random.permutation)(row_keys, parents)
    octants = jax.random.randint(octant_key, (DEVICES, CAP), 0, 8)
    return (parents * 8 + octants).reshape(DEVICES * CAP).astype(jnp.int32)


def route_plan(key):
    base_key = jax.random.fold_in(key, 37)
    start_key, pair_key, section_key = jax.random.split(base_key, 3)
    quarter = CAP // 4
    live_now = jax.random.randint(start_key, (DEVICES,), quarter, 3 * quarter + 1)
    half_way = DEVICES // 2
    chosen = jax.random.randint(pair_key, (), 0, half_way)
    live_now = live_now.at[chosen].set(3 * quarter).at[chosen + half_way].set(3 * quarter)
    initial = live_now
    everyone = jnp.arange(DEVICES, dtype=jnp.int32)
    outer_bits = int(N_GX).bit_length() - 1
    middle_bits = int(N_GY).bit_length() - 1
    phase_firsts = [0, outer_bits, outer_bits + middle_bits]
    sender = chosen.astype(jnp.int32)
    holder = (chosen + half_way).astype(jnp.int32)
    count_rows = []
    for section_num in range(SECTIONS):
        bit_mask = 1 << SECTIONS - 1 - section_num
        partner = jnp.bitwise_xor(everyone, bit_mask)
        lower_half = jnp.bitwise_and(everyone, bit_mask) == 0
        phase_start = section_num in phase_firsts
        if phase_start and section_num > 0:
            sender = jnp.argmax(live_now).astype(jnp.int32)
            holder = jnp.bitwise_xor(sender, bit_mask)
        is_sender = everyone == sender
        is_holder = everyone == holder
        low_key, high_key = jax.random.split(jax.random.fold_in(section_key, section_num))
        low_count = jax.random.randint(low_key, (DEVICES,), 0, jnp.minimum(live_now, SEND_CAP) + 1)
        if phase_start:
            low_count = jnp.where(is_sender, SEND_CAP, low_count)
            low_count = jnp.where(is_holder, jnp.maximum(low_count, live_now + SEND_CAP - CAP), low_count)
        else:
            spare_room = CAP - live_now[holder]
            low_count = jnp.where(is_holder, 0, low_count)
            low_count = jnp.where(partner == holder, jnp.minimum(low_count, spare_room), low_count)
        paired_count = low_count[partner]
        held_count = live_now[partner]
        lowest = jnp.maximum(0, live_now + paired_count - CAP)
        highest = jnp.maximum(lowest, jnp.minimum(jnp.minimum(live_now, SEND_CAP), CAP - held_count + paired_count))
        high_count = jax.random.randint(high_key, (DEVICES,), lowest, highest + 1)
        if phase_start:
            high_count = jnp.where(is_sender, SEND_CAP, high_count)
        else:
            high_count = jnp.where(is_holder, 0, high_count)
        if section_num == 0:
            high_count = jnp.where(is_holder, 0, high_count)
        counts = jnp.where(lower_half, low_count, high_count)
        count_rows.append(counts)
        live_now = live_now - counts + counts[partner]
    return (initial.astype(jnp.int32), jnp.stack(count_rows).astype(jnp.int32))


def draw_leaf_ids(key, part):
    return leaf_table(key)


def draw_live_counts(key, part):
    return route_plan(key)[0]


def draw_send_counts(key, part):
    return route_plan(key)[1]


def draw_positions(key, part):
    leaves = leaf_table(key)
    coordinates = []
    for axis_bit in (2, 1, 0):
        coordinate = jnp.zeros_like(leaves)
        for level_num in range(LEVEL):
            octant_id = jnp.right_shift(leaves, 3 * level_num)
            coordinate = coordinate + jnp.left_shift(jnp.bitwise_and(jnp.right_shift(octant_id, axis_bit), 1), level_num)
        coordinates.append(coordinate.astype(jnp.float32))
    cell_grid = jnp.stack(coordinates)
    fraction = jax.random.uniform(jax.random.fold_in(key, 23), (3, DEVICES * CAP, PART), jnp.float32, 0.0, 1.0)
    fraction = 0.001 + 0.998 * fraction
    return ((cell_grid[:, :, None] + fraction) / float(2 ** LEVEL)).astype(jnp.float32)


def level_of(own_key, dims, cuts, low, largest):
    loudness, own = 1.0, jax.random.fold_in(own_key, 6)
    for axis_at, blocks in cuts:
        heights = jnp.exp(jax.random.uniform(jax.random.fold_in(own, axis_at), (blocks,), jnp.float32, low / len(cuts), largest / len(cuts)))
        loudness = loudness * jnp.repeat(heights, dims[axis_at] // blocks).reshape([-1 if axis == axis_at else 1 for axis in range(len(dims))])
    return loudness


def noise(own_key, shape, deviation, bound, cuts=(), kind=jnp.bfloat16):
    factor_of = level_of(own_key, shape, cuts, -0.22, 0.18) if cuts else 1.0
    entries = jax.random.normal(own_key, shape, jnp.float32) * deviation * factor_of
    return jnp.minimum(jnp.maximum(entries, -bound), bound).astype(kind)


def setup_inputs(seed: int = 0) -> dict:
    streams_of = jax.random.split(jax.random.key(seed), 7)
    positions = draw_positions(jax.random.fold_in(streams_of[6], 71), 0)
    charges = noise(streams_of[1], (BLOCKS, PART), 1.0, 6.0, ((0, 32),), jnp.float32)
    velocities = noise(streams_of[2], (3, BLOCKS, PART), 1.0, 6.0, ((1, 32),), jnp.float32)
    leaf_ids = draw_leaf_ids(jax.random.fold_in(streams_of[6], 71), 0)
    live_counts = draw_live_counts(jax.random.fold_in(streams_of[6], 71), 0)
    send_counts = draw_send_counts(jax.random.fold_in(streams_of[6], 71), 0)
    return dict(positions=positions, charges=charges, velocities=velocities, leaf_ids=leaf_ids, live_counts=live_counts, send_counts=send_counts)


def exponents(max_order):
    return [(p, q, r) for p in range(max_order + 1) for q in range(max_order + 1 - p) for r in range(max_order + 1 - p - q)]


def shift_tables(max_order):
    triples = exponents(max_order)
    count = len(triples)
    tables = np.zeros((8, count, count))
    for octant_id in range(8):
        signs = [0.5 if (octant_id >> shift_bit) & 1 else -0.5 for shift_bit in (2, 1, 0)]
        for k, (p, q, r) in enumerate(triples):
            for j, (e, f, g) in enumerate(triples):
                if e <= p and f <= q and g <= r:
                    tables[octant_id, k, j] = (math.comb(p, e) * math.comb(q, f) * math.comb(r, g)
                                               * signs[0] ** (p - e) * signs[1] ** (q - f) * signs[2] ** (r - g)
                                               * 0.5 ** (e + f + g))
    return jnp.asarray(tables, jnp.float32)


def morton_cells(leaves, tree_depth):
    coordinates = []
    for axis_bit in (2, 1, 0):
        coordinate = jnp.zeros_like(leaves)
        for level_num in range(tree_depth):
            octant_id = jnp.right_shift(leaves, 3 * level_num)
            coordinate = coordinate + jnp.left_shift(jnp.bitwise_and(jnp.right_shift(octant_id, axis_bit), 1), level_num)
        coordinates.append(coordinate)
    return coordinates


def leaf_moments(positions, charges, leaves, max_order, tree_depth):
    cells_side = float(2 ** tree_depth)
    coordinates = morton_cells(leaves, tree_depth)
    powers = []
    for axis_num in range(3):
        offset_row = 2.0 * (positions[axis_num] * cells_side - coordinates[axis_num].astype(jnp.float32)[:, None]) - 1.0
        power_list = [jnp.ones_like(offset_row)]
        for degree_num in range(max_order):
            power_list.append(power_list[-1] * offset_row)
        powers.append(power_list)
    exponent_pairs = [(p, q) for p in range(max_order + 1) for q in range(max_order + 1 - p)]
    weighted = jnp.stack([charges * powers[0][p] * powers[1][q] for p, q in exponent_pairs])
    third_powers = jnp.stack(powers[2])
    raw_sums = jnp.einsum('pbi,cbi->pcb', weighted, third_powers, precision=lax.Precision.HIGHEST)
    pieces = [raw_sums[n, :max_order + 1 - p - q] for n, (p, q) in enumerate(exponent_pairs)]
    return jnp.concatenate(pieces, axis=0) / 16.0


def parent_moments(moments, leaves, live_mask, tables):
    shifted = jnp.einsum('okj,jb->okb', tables, moments, precision=lax.Precision.HIGHEST)
    octant_id = jnp.bitwise_and(leaves, 7)
    chooser = (octant_id[None, :] == jnp.arange(8, dtype=jnp.int32)[:, None]).astype(jnp.float32)
    moved = jnp.sum(shifted * chooser[:, None, :], axis=0)
    parents = jnp.right_shift(leaves, 3)
    sibling = ((parents[:, None] == parents[None, :]) & live_mask[:, None] & live_mask[None, :]).astype(jnp.float32)
    return jnp.dot(moved, sibling, precision=lax.Precision.HIGHEST, preferred_element_type=jnp.float32)


def outgoing(blocks_now, live_count, sent_count, upper_half, slab_rows):
    start_at = jnp.where(upper_half, 0, live_count - sent_count).astype(jnp.int32)

    def cut(member):
        padding = jnp.zeros(member.shape[:1] + (slab_rows,) + member.shape[2:], member.dtype)
        return lax.dynamic_slice_in_dim(jnp.concatenate([member, padding], axis=1), start_at, slab_rows, 1)

    return jax.tree.map(cut, blocks_now)


def incoming(blocks_now, arrived, live_count, sent_count, got_count, upper_half):
    kept_count = live_count - sent_count

    def place(member, slab_part):
        slot_total = member.shape[1]
        slab_rows = slab_part.shape[1]
        edge_pad = jnp.zeros(member.shape[:1] + (slab_rows,) + member.shape[2:], member.dtype)
        wide_pad = jnp.zeros(member.shape, member.dtype)
        offset_old = jnp.where(upper_half, sent_count - got_count, 0)
        shifted = lax.dynamic_slice_in_dim(jnp.concatenate([edge_pad, member, edge_pad], axis=1),
                                           (slab_rows + offset_old).astype(jnp.int32), slot_total, 1)
        offset_new = jnp.where(upper_half, 0, kept_count)
        placed = lax.dynamic_slice_in_dim(jnp.concatenate([wide_pad, slab_part, wide_pad], axis=1),
                                          (slot_total - offset_new).astype(jnp.int32), slot_total, 1)
        slot_ids = jnp.arange(slot_total, dtype=jnp.int32)
        take_new = jnp.where(upper_half, slot_ids < got_count, (slot_ids >= kept_count) & (slot_ids < kept_count + got_count))
        take_old = jnp.where(upper_half, (slot_ids >= got_count) & (slot_ids < got_count + kept_count), slot_ids < kept_count)
        shape_mask = (1, slot_total) + (1,) * (member.ndim - 2)
        take_new = take_new.reshape(shape_mask)
        take_old = take_old.reshape(shape_mask)
        return jnp.where(take_new, placed, jnp.where(take_old, shifted, jnp.zeros_like(member)))

    return jax.tree.map(place, blocks_now, arrived)


def reference(positions, charges, velocities, leaf_ids, live_counts, send_counts):
    blocks_now = (jnp.moveaxis(positions.reshape(3, DEVICES, CAP, PART), 1, 0),
                  charges.reshape(DEVICES, 1, CAP, PART),
                  jnp.moveaxis(velocities.reshape(3, DEVICES, CAP, PART), 1, 0),
                  leaf_ids.astype(jnp.float32).reshape(DEVICES, 1, CAP))
    everyone = jnp.arange(DEVICES, dtype=jnp.int32)
    live_all = live_counts
    send_out = partial(outgoing, slab_rows=SEND_CAP)
    for section_num in range(SECTIONS):
        bit_mask = 1 << (SECTIONS - 1 - section_num)
        partner = jnp.bitwise_xor(everyone, bit_mask)
        upper_half = jnp.bitwise_and(everyone, bit_mask) != 0
        sent_count = send_counts[section_num]
        got_count = sent_count[partner]
        outbound = jax.vmap(send_out)(blocks_now, live_all, sent_count, upper_half)
        arrived = jax.tree.map(lambda member: member[partner], outbound)
        blocks_now = jax.vmap(incoming)(blocks_now, arrived, live_all, sent_count, got_count, upper_half)
        live_all = live_all - sent_count + got_count
    tables = shift_tables(ORDER)

    def settle(inputs):
        device_positions, device_charges, device_leaves, live_count = inputs
        live_mask = jnp.arange(CAP, dtype=jnp.int32) < live_count
        leaves = jnp.where(live_mask, device_leaves[0].astype(jnp.int32), 0)
        leaf_part = leaf_moments(device_positions, device_charges[0], leaves, ORDER, LEVEL)
        return leaf_part, parent_moments(leaf_part, leaves, live_mask, tables)

    leaf_part, parent_part = lax.map(settle, (blocks_now[0], blocks_now[1], blocks_now[3], live_all))
    all_mask = jnp.arange(CAP, dtype=jnp.int32)[None, :] < live_all[:, None]
    moved_leaves = jnp.where(all_mask, blocks_now[3][:, 0].astype(jnp.int32), -1).reshape(BLOCKS)
    moved_positions = jnp.moveaxis(blocks_now[0], 0, 1).reshape(3, BLOCKS, PART)
    moved_charges = blocks_now[1].reshape(BLOCKS, PART)
    moved_velocities = jnp.moveaxis(blocks_now[2], 0, 1).reshape(3, BLOCKS, PART)
    first_out = jnp.moveaxis(leaf_part, 0, 1).reshape(NCOEF, BLOCKS)
    second_out = jnp.moveaxis(parent_part, 0, 1).reshape(NCOEF, BLOCKS)
    return (moved_positions, moved_charges, moved_velocities, moved_leaves, first_out, second_out)
```

```python
import functools
import math

import jax
import jax.numpy as jnp
import numpy as np
from jax import lax
from jax.experimental import pallas as pl
from jax.experimental.pallas import tpu as pltpu
from jax.sharding import PartitionSpec as P

ORDER = 10
LEVEL = 7
AXES = ("gx", "gy", "gz")
FIELDS = 6
LANES = 128


def exponents(order):
    return [
        (p, q, r)
        for p in range(order + 1)
        for q in range(order + 1 - p)
        for r in range(order + 1 - p - q)
    ]


def up8(count):
    return -(-count // 8) * 8


def shift_matrix(order):
    triples = exponents(order)
    size = up8(len(triples))
    table = np.zeros((size, size))
    for k, (p, q, r) in enumerate(triples):
        for j, (e, f, g) in enumerate(triples):
            if e <= p and f <= q and g <= r:
                ways = math.comb(p, e) * math.comb(q, f) * math.comb(r, g)
                table[k, j] = ways * 0.5 ** (p + q + r)
    out = table.astype(jnp.bfloat16)
    assert (out.astype(np.float64) == table).all()
    return out


def sign_matrix(order):
    triples = exponents(order)
    table = np.zeros((up8(len(triples)), LANES))
    for k, (p, q, r) in enumerate(triples):
        for octant in range(8):
            sx, sy, sz = [1 if octant >> t & 1 else -1 for t in (2, 1, 0)]
            table[k, octant] = sx**p * sy**q * sz**r
    return table.astype(jnp.bfloat16)


class Plan:
    def __init__(self, mesh, slots):
        self.devices = math.prod(mesh.shape[a] for a in AXES)
        self.sections = self.devices.bit_length() - 1
        self.slots = slots
        self.slab = slots // 4
        self.first = self.sections * self.slab
        self.rows = slots + 2 * self.first

    def mask(self, section):
        return 1 << (self.sections - 1 - section)


def my_index():
    index = lax.axis_index(AXES[0])
    for axis in AXES[1:]:
        index = index * lax.axis_size(axis) + lax.axis_index(axis)
    return index


def route(plan, me, live_ref, send_ref):
    base = jnp.int32(plan.first)
    count = live_ref[me]
    values = []
    for section in range(plan.sections):
        mask = plan.mask(section)
        upper = jnp.bitwise_and(me, mask) != 0
        sent = send_ref[section, me]
        got = send_ref[section, jnp.bitwise_xor(me, mask)]
        kept = count - sent
        start = jnp.where(upper, 0, kept)
        turn = jnp.where(upper, got - sent, kept)
        values += [
            jnp.where(upper, base, base + count - plan.slab),
            jnp.where(upper, base + sent - plan.slab, base + kept),
            jnp.bitwise_and(LANES - start, LANES - 1),
            jnp.bitwise_and(turn + LANES, LANES - 1),
            jnp.where(upper, got, kept),
            jnp.where(upper, 1, 0),
        ]
        base = jnp.where(upper, base + sent - got, base)
        count = kept + got
    return values + [base, count]


def field(plan_ref, section, number):
    return plan_ref[0, section * FIELDS + number]


def leaf_out(plan_ref, section, row):
    return pltpu.roll(row, field(plan_ref, section, 2), 1)


def leaf_in(plan_ref, section, row, new):
    lane = lax.broadcasted_iota(jnp.int32, row.shape, 1)
    upper = field(plan_ref, section, 5) != 0
    turned = pltpu.roll(jnp.where(upper, row, new), field(plan_ref, section, 3), 1)
    return jnp.where(lane < field(plan_ref, section, 4), jnp.where(upper, new, row), turned)


def cut(plan, state_ref, at, slab_ref):
    size = plan.slab
    for c in range(state_ref.shape[0]):
        slab_ref[pl.ds(c * size, size), :] = state_ref[c, pl.ds(at, size), :]


def first_kernel(
    plan, live_hbm, send_hbm, pos, chg, leaf_hbm, slab_ref, state_ref, row_ref, plan_ref,
    live_ref, send_ref, leaf_ref, sems,
):
    window = pl.ds(plan.first, plan.slots)
    copies = [
        pltpu.make_async_copy(live_hbm, live_ref, sems.at[0]),
        pltpu.make_async_copy(send_hbm, send_ref, sems.at[1]),
        pltpu.make_async_copy(leaf_hbm, leaf_ref, sems.at[2]),
        pltpu.make_async_copy(pos, state_ref.at[pl.ds(0, 3), window, :], sems.at[3]),
        pltpu.make_async_copy(chg, state_ref.at[3, window, :], sems.at[4]),
    ]
    for copy in copies:
        copy.start()
    copies[0].wait()
    copies[1].wait()
    values = route(plan, my_index(), live_ref, send_ref)
    lane = lax.broadcasted_iota(jnp.int32, (8, LANES), 1)
    table = jnp.zeros((8, LANES), jnp.int32)
    for number, value in enumerate(values):
        table = jnp.where(lane == number, value, table)
    plan_ref[...] = table
    copies[2].wait()
    row = jnp.broadcast_to(leaf_ref[...].astype(jnp.float32), (8, LANES))
    row_ref[...] = row
    slab_ref[pl.ds(4 * plan.slab, 8), :] = pltpu.roll(row, values[2], 1)
    copies[3].wait()
    copies[4].wait()
    cut(plan, state_ref, values[0], slab_ref)


def first_velocities(plan, plan_ref, vel, slab_ref, state_ref, sem):
    copy = pltpu.make_async_copy(
        vel, state_ref.at[:, pl.ds(plan.first, plan.slots), :], sem
    )
    copy.start()
    copy.wait()
    cut(plan, state_ref, field(plan_ref, 0, 0), slab_ref)


def next_slab(plan, section, plan_ref, state_ref, arr_ref, slab_ref, near_ref):
    size = plan.slab
    at = field(plan_ref, section + 1, 0)
    over = jnp.clip(field(plan_ref, section, 1) - at + size, 0, 2 * size)
    for c in range(state_ref.shape[0]):
        near_ref[c, pl.ds(size, size), :] = state_ref[c, pl.ds(at, size), :]
        near_ref[c, pl.ds(over, size), :] = arr_ref[pl.ds(c * size, size), :]
        slab_ref[pl.ds(c * size, size), :] = near_ref[c, pl.ds(size, size), :]


def slab_kernel(plan, section, plan_ref, state_ref, arr_ref, row_ref, slab_ref, row_out, near_ref):
    next_slab(plan, section, plan_ref, state_ref, arr_ref, slab_ref, near_ref)
    tail = pl.ds(4 * plan.slab, 8)
    row = leaf_in(plan_ref, section, row_ref[...], arr_ref[tail, :])
    row_out[...] = row
    slab_ref[tail, :] = leaf_out(plan_ref, section + 1, row)


def overlay(plan, section, plan_ref, arr_ref, state_ref):
    size = plan.slab
    at = field(plan_ref, section, 1)
    for c in range(state_ref.shape[0]):
        state_ref[c, pl.ds(at, size), :] = arr_ref[pl.ds(c * size, size), :]


def merge_kernel(plan, section, plan_ref, state_in, arr_ref, state_ref):
    state_ref[...] = state_in[...]
    overlay(plan, section, plan_ref, arr_ref, state_ref)


def settled(plan, plan_ref, state_in, arr_ref, work_ref):
    last = plan.sections - 1
    slots = plan.slots
    base = field(plan_ref, last + 1, 0)
    count = field(plan_ref, last + 1, 1)
    work_ref[...] = state_in[...]
    overlay(plan, last, plan_ref, arr_ref, work_ref)
    live = lax.broadcasted_iota(jnp.int32, (slots, LANES), 0) < count
    for c in range(state_in.shape[0]):
        yield c, jnp.where(live, work_ref[c, pl.ds(base, slots), :], 0.0)


def split3(value):
    high = value.astype(jnp.bfloat16)
    rest = value - high.astype(jnp.float32)
    mid = rest.astype(jnp.bfloat16)
    low = (rest - mid.astype(jnp.float32)).astype(jnp.bfloat16)
    return high, mid, low


def cell_rows(leaves):
    rows = []
    for axis_bit in (2, 1, 0):
        cell = jnp.zeros_like(leaves)
        for t in range(LEVEL):
            bit = jnp.bitwise_and(jnp.right_shift(leaves, 3 * t + axis_bit), 1)
            cell = cell + jnp.left_shift(bit, t)
        rows.append(cell.astype(jnp.float32))
    return rows


def final_leaves(plan, plan_ref, row):
    lane = lax.broadcasted_iota(jnp.int32, (8, LANES), 1)
    live = lane < field(plan_ref, plan.sections, 1)
    return live, jnp.where(live, row.astype(jnp.int32), 0)


def moments_kernel(
    plan, plan_ref, state_in, arr_ref, row_ref, out_pos, out_chg, row_out, mom_ref,
    work_ref, parts_ref, axis_ref, kept_ref, sems,
):
    row = leaf_in(plan_ref, plan.sections - 1, row_ref[...], arr_ref[pl.ds(4 * plan.slab, 8), :])
    row_out[...] = row
    _, leaves = final_leaves(plan, plan_ref, row)
    cells = cell_rows(leaves)
    side = float(2**LEVEL)
    for c, value in settled(plan, plan_ref, state_in, arr_ref, work_ref):
        kept_ref[c] = value
        turned = value.T
        if c < 3:
            turned = 2.0 * (turned * side - cells[c][:1]) - 1.0
        axis_ref[c] = turned
    copies = [
        pltpu.make_async_copy(kept_ref.at[pl.ds(0, 3)], out_pos, sems.at[0]),
        pltpu.make_async_copy(kept_ref.at[3], out_chg, sems.at[1]),
    ]
    for copy in copies:
        copy.start()
    chunks = plan.slots // 8
    triples = exponents(ORDER)
    place = {t: k for k, t in enumerate(triples)}
    for p in range(ORDER + 1):
        for q in range(ORDER + 1 - p):
            top = ORDER + 1 - p - q
            sums = [None] * top
            for g in range(chunks):
                rows = pl.ds(g * 8, 8)
                if q == 0:
                    term = axis_ref[3, rows, :]
                    if p > 0:
                        term = term * axis_ref[0, rows, :]
                        axis_ref[3, rows, :] = term
                else:
                    term = axis_ref[4, rows, :] * axis_ref[1, rows, :]
                axis_ref[4, rows, :] = term
                w = axis_ref[2, rows, :]
                for r in range(top):
                    sums[r] = term if g == 0 else sums[r] + term
                    if r + 1 < top:
                        term = term * w
            for r in range(top):
                parts_ref[pl.ds(place[p, q, r] * 8, 8), :] = sums[r]
    size = mom_ref.shape[0]
    for k in range(len(triples), size):
        parts_ref[pl.ds(k * 8, 8), :] = jnp.zeros((8, LANES), jnp.float32)
    for g in range(size // 8):
        total = parts_ref[pl.ds(g * 64, 8, stride=8), :]
        for s in range(1, 8):
            total = total + parts_ref[pl.ds(g * 64 + s, 8, stride=8), :]
        mom_ref[pl.ds(g * 8, 8), :] = total * (1.0 / 16.0)
    for copy in copies:
        copy.wait()


def parents_kernel(
    plan, plan_ref, state_in, arr_ref, row_ref, mom_ref, shift_ref, sign_ref,
    out_vel, out_leaf, out_mom, out_par, work_ref, kept_ref, par_ref, leaf_ref, sems,
):
    rows = out_mom.shape[0]
    copies = [pltpu.make_async_copy(mom_ref.at[pl.ds(0, rows)], out_mom, sems.at[0])]
    copies[-1].start()
    for c, value in settled(plan, plan_ref, state_in, arr_ref, work_ref):
        kept_ref[c] = value
    copies.append(pltpu.make_async_copy(kept_ref, out_vel, sems.at[1]))
    copies[-1].start()
    live, leaves = final_leaves(plan, plan_ref, row_ref[...])
    leaf_ref[...] = jnp.where(live, leaves, -1)[:1]
    copies.append(pltpu.make_async_copy(leaf_ref, out_leaf, sems.at[2]))
    copies[-1].start()
    lane = lax.broadcasted_iota(jnp.int32, (8, LANES), 1)
    octant = jnp.bitwise_and(leaves, 7)
    chooser = lax.broadcasted_iota(jnp.int32, (LANES, LANES), 0) == octant[:1]
    chooser = jnp.where(chooser, 1.0, 0.0).astype(jnp.bfloat16)
    signs = jnp.dot(sign_ref[...], chooser, preferred_element_type=jnp.float32)
    pieces = split3(mom_ref[...] * signs)
    shift = shift_ref[...]
    shifted = sum(jnp.dot(shift, piece, preferred_element_type=jnp.float32) for piece in pieces)
    moved = shifted * signs
    key = jnp.where(live, jnp.right_shift(leaves, 3), -1 - lane).astype(jnp.float32)
    key_row = jnp.broadcast_to(key[:1], (LANES, LANES))
    sibling = jnp.where(key_row.T == key_row, 1.0, 0.0).astype(jnp.bfloat16)
    par_ref[...] = sum(
        jnp.dot(piece, sibling, preferred_element_type=jnp.float32) for piece in split3(moved)
    )
    copies.append(pltpu.make_async_copy(par_ref.at[pl.ds(0, rows)], out_par, sems.at[3]))
    copies[-1].start()
    for copy in copies:
        copy.wait()


VMEM = pl.BlockSpec(memory_space=pltpu.VMEM)
HBM = pl.BlockSpec(memory_space=pltpu.HBM)


def call(body, outs, ins, out_specs, in_specs, scratch, flops, name):
    return pl.pallas_call(
        body,
        out_shape=outs,
        in_specs=in_specs,
        out_specs=out_specs,
        scratch_shapes=scratch,
        compiler_params=pltpu.CompilerParams(vmem_limit_bytes=8 << 20),
        cost_estimate=pl.CostEstimate(flops=flops, bytes_accessed=flops, transcendentals=0),
        name=name,
    )(*ins)


def per_device(plan, positions, charges, velocities, leaf_ids, live_counts, send_counts):
    f32 = jnp.float32
    shape = jax.ShapeDtypeStruct
    slots, size, last = plan.slots, plan.slab, plan.sections - 1
    dma = pltpu.SemaphoreType.DMA
    row_shape = shape((8, LANES), f32)

    def slab_shape(planes):
        return shape((planes * size + (8 if planes == 4 else 0), LANES), f32)

    def state_shape(planes):
        return shape((planes, plan.rows, LANES), f32)

    def near(planes):
        return pltpu.VMEM((planes, 3 * size, LANES), f32)

    def swap(slab, section):
        mask = plan.mask(section)
        return lax.ppermute(slab, AXES, [(d, d ^ mask) for d in range(plan.devices)])

    def at_home(value):
        return pltpu.with_memory_space_constraint(value, pltpu.HBM)

    slab, state, row, table = call(
        functools.partial(first_kernel, plan),
        (slab_shape(4), state_shape(4), row_shape, shape((8, LANES), jnp.int32)),
        tuple(map(at_home, (live_counts, send_counts, positions, charges, leaf_ids.reshape(1, LANES)))),
        (VMEM,) * 4, (HBM,) * 5,
        [
            pltpu.SMEM(live_counts.shape, jnp.int32),
            pltpu.SMEM(send_counts.shape, jnp.int32),
            pltpu.VMEM((1, LANES), jnp.int32),
            dma((5,)),
        ],
        1 << 20, "first",
    )
    arrived = swap(slab, 0)
    vslab, vstate = call(
        functools.partial(first_velocities, plan),
        (slab_shape(3), state_shape(3)), (table, at_home(velocities)),
        (VMEM, VMEM), (VMEM, HBM), [dma], 1 << 20, "first_vel",
    )
    varrived = swap(vslab, 0)
    for section in range(last):
        slab, row = call(
            functools.partial(slab_kernel, plan, section),
            (slab_shape(4), row_shape), (table, state, arrived, row),
            (VMEM, VMEM), (VMEM,) * 4, [near(4)], 1 << 18, f"slab{section}",
        )
        after = swap(slab, section + 1)
        state = call(
            functools.partial(merge_kernel, plan, section),
            state_shape(4), (table, state, arrived), VMEM, (VMEM,) * 3, [], 1 << 18, f"merge{section}",
        )
        vslab = call(
            functools.partial(next_slab, plan, section),
            slab_shape(3), (table, vstate, varrived),
            VMEM, (VMEM,) * 3, [near(3)], 1 << 18, f"vslab{section}",
        )
        vafter = swap(vslab, section + 1)
        vstate = call(
            functools.partial(merge_kernel, plan, section),
            state_shape(3), (table, vstate, varrived), VMEM, (VMEM,) * 3, [], 1 << 18, f"vmerge{section}",
        )
        arrived, varrived = after, vafter
    count = len(exponents(ORDER))
    rows = up8(count)
    pos, chg, row, moments = call(
        functools.partial(moments_kernel, plan),
        (shape(positions.shape, f32), shape(charges.shape, f32), row_shape, shape((rows, LANES), f32)),
        (table, state, arrived, row),
        (HBM, HBM, VMEM, VMEM), (VMEM,) * 4,
        [
            pltpu.VMEM((4, plan.rows, LANES), f32),
            pltpu.VMEM((rows * 8, LANES), f32),
            pltpu.VMEM((5, LANES, LANES), f32),
            pltpu.VMEM((4, slots, LANES), f32),
            dma((2,)),
        ],
        1 << 26, "moments",
    )
    vel, leaves, leaf_part, parent_part = call(
        functools.partial(parents_kernel, plan),
        (
            shape(velocities.shape, f32),
            shape((1, LANES), jnp.int32),
            shape((count, LANES), f32),
            shape((count, LANES), f32),
        ),
        (
            table, vstate, varrived, row, moments,
            jnp.asarray(shift_matrix(ORDER)), jnp.asarray(sign_matrix(ORDER)),
        ),
        (HBM,) * 4, (VMEM,) * 7,
        [
            pltpu.VMEM((3, plan.rows, LANES), f32),
            pltpu.VMEM((3, slots, LANES), f32),
            pltpu.VMEM((rows, LANES), f32),
            pltpu.VMEM((1, LANES), jnp.int32),
            dma((4,)),
        ],
        1 << 26, "parents",
    )
    return pos, chg, vel, leaves.reshape(LANES), leaf_part, parent_part


def solution(mesh):
    def body(positions, *rest):
        return per_device(Plan(mesh, positions.shape[1]), positions, *rest)

    blocks = (P(None, AXES, None), P(AXES, None), P(None, AXES, None), P(AXES))
    return jax.shard_map(
        body,
        mesh=mesh,
        in_specs=blocks + (P(), P()),
        out_specs=blocks + (P(None, AXES), P(None, AXES)),
        check_vma=False,
    )
```
